256 devices in a mesh: gx: 32 (over x_lo, z, core), gy: 8 (over y, x_hi).
Axes of the slice: x: 4 (x_hi: 2, x_lo: 2; x = x_hi * 2 + x_lo), y: 4, z: 8, core: 2. Of those that a mesh axis runs over, the one named last changes fastest.
Arguments:
- adjoint: bfloat16 [512, 1024, 512], P('gx', 'gy'), may hold values from -6 to 6
- conduct_x: float32 [512, 1024], P('gx', 'gy'), may hold values from 0.02 to 0.24
- conduct_y: float32 [512, 1024], P('gx', 'gy'), may hold values from 0.02 to 0.24
- pick_weights: bfloat16 [512, 512, 1024], P(None, 'gx', 'gy'), may hold values from -0.015625 to 0.015625
- owner_order: int32 [512], replicated, may hold values from 0 to 511, each once
Outputs:
- smoothed: bfloat16 [512, 1024, 512], P('gx', 'gy')
- representer: float32 [512, 512], P(('gx', 'gy'))
The draws below stay inside these ranges and needn't reach their ends.
Inputs may be any that keep to these rules, and one draw needn't show every extreme that they name: `owner_order`: each of 0 to 511 appears once.
All inputs are finite; a program needn't handle non-finite values.
Results may differ from the reference program's by a relative error of at most 0.0029.
Values may be sent and summed in bfloat16 or wider, within the bound.
No kernel may reach another device: no remote copies, remote signals or barrier semaphores. Data moves between devices by JAX's collectives and lax.ppermute only.
A program may use at most 64 MiB of HBM per device.

```python
import math
import jax
import jax.numpy as jnp

PANEL = 256
PANELS = 2
STEPS = 4
COLUMNS = 512
PICKS = 512
NX = 512
NY = 1024


def raised(entries, stream_key, source, target, shards_of, factor):
    owner, partner = [(jnp.arange(entries.shape[axis_at]) // (entries.shape[axis_at] // shards_of)).reshape([-1 if axis == axis_at else 1 for axis in range(entries.ndim)]) for axis_at in (source, target)]
    chosen = jax.random.permutation(stream_key, shards_of)[partner]
    strong = (owner == chosen) | (owner == (partner + shards_of // 2) % shards_of)
    return jnp.where(strong, factor * entries, entries)


def shard_levels(stream_key, dims, shards, smallest, largest):
    level = 1.0
    for axis_at, shards_of in shards:
        steps = jax.random.uniform(jax.random.fold_in(jax.random.fold_in(stream_key, 6), axis_at), (shards_of,), jnp.float32, smallest / len(shards), largest / len(shards))
        level = level * jnp.repeat(jnp.exp(steps), dims[axis_at] // shards_of).reshape((-1,) + (1,) * (len(dims) - 1 - axis_at))
    return level


def normal_values(stream_key, extent, deviation, reach, split=(), kind=jnp.bfloat16):
    values = deviation * jax.random.normal(stream_key, extent, jnp.float32)
    if split:
        values = values * shard_levels(stream_key, extent, split, -0.22, 0.18)
    return jnp.clip(values, -reach, reach).astype(kind)


def bell_draw_with(rng, extent, deviation, reach, split, heavy, kind=jnp.bfloat16):
    drawn = deviation * jax.random.normal(rng, extent, jnp.float32)
    if split:
        drawn = drawn * shard_levels(rng, extent, split, -0.22, 0.18)
    return jnp.clip(raised(drawn, jax.random.fold_in(rng, 3), *heavy), -reach, reach).astype(kind)


def setup_inputs(seed: int = 0) -> dict:
    splits = jax.random.split(jax.random.key(seed), 6)
    return {
        "adjoint": normal_values(splits[0], (NX, NY, COLUMNS), 1.0, 6.0, ((0, 32), (1, 8))),
        "conduct_x": jnp.clip(jnp.exp(math.log(0.24) - 2.4849066 * jax.random.uniform(splits[1], (NX, NY), jnp.float32) ** shard_levels(splits[1], (NX, NY), ((0, 32), (1, 8)), -0.2, 0.2)), 0.02, 0.24),
        "conduct_y": jnp.clip(jnp.exp(math.log(0.24) - 2.4849066 * jax.random.uniform(splits[2], (NX, NY), jnp.float32) ** shard_levels(splits[2], (NX, NY), ((0, 32), (1, 8)), -0.2, 0.2)), 0.02, 0.24),
        "pick_weights": bell_draw_with(splits[3], (PICKS, NX, NY), (NX * NY) ** -0.5, 0.015625, ((1, 32), (2, 8)), (1, 0, 32, 2.75)),
        "owner_order": jax.random.permutation(splits[4], PICKS).astype(jnp.int32),
    }


def diffuse(field, conx, cony):
    centre = field[1:-1, 1:-1]
    above = field[:-2, 1:-1]
    below = field[2:, 1:-1]
    leftside = field[1:-1, :-2]
    rightside = field[1:-1, 2:]
    result = centre + conx[:-2, 1:-1, None] * (above - centre)
    result = result + conx[1:-1, 1:-1, None] * (below - centre)
    result = result + cony[1:-1, :-2, None] * (leftside - centre)
    result = result + cony[1:-1, 1:-1, None] * (rightside - centre)
    return result


def reference(adjoint, conduct_x, conduct_y, pick_weights, owner_order):
    rows_idx = jnp.arange(NX, dtype=jnp.int32)[:, None]
    cols_idx = jnp.arange(NY, dtype=jnp.int32)[None, :]
    conx = jnp.where(rows_idx < NX - 1, conduct_x, jnp.float32(0.0))
    cony = jnp.where(cols_idx < NY - 1, conduct_y, jnp.float32(0.0))
    conx_pad = jnp.pad(conx, 1)
    cony_pad = jnp.pad(cony, 1)
    flat_weights = pick_weights.reshape(PICKS, NX * NY)
    smooth_list = []
    repr_list = []
    for panel in range(PANELS):
        field = adjoint[:, :, panel * PANEL:(panel + 1) * PANEL].astype(jnp.float32)
        for step in range(STEPS):
            field = diffuse(jnp.pad(field, ((1, 1), (1, 1), (0, 0))), conx_pad, cony_pad)
        rounded = field.astype(jnp.bfloat16)
        smooth_list.append(rounded)
        partial_value = jnp.dot(flat_weights, rounded.reshape(NX * NY, PANEL), preferred_element_type=jnp.float32)
        repr_list.append(jnp.take(partial_value, owner_order, axis=0))
    return jnp.concatenate(smooth_list, axis=2), jnp.concatenate(repr_list, axis=1)
```

```python
import jax
import jax.numpy as jnp
from jax import lax
from jax.experimental import pallas as pl
from jax.experimental.pallas import tpu as pltpu
from jax.sharding import Mesh
from jax.sharding import PartitionSpec as P

STEPS = 4
BF = jnp.bfloat16
F32 = jnp.float32
VMEM = pl.BlockSpec(memory_space=pltpu.VMEM)
SMEM = pl.BlockSpec(memory_space=pltpu.SMEM)
HBM = pl.BlockSpec(memory_space=pltpu.HBM)
MIB = 1024 * 1024
ALONG = ("g", "core")
PITCH = 520


def parity_x():
    return lax.axis_index("core")


def parity_y():
    return lax.rem(lax.axis_index("gy"), 2)


def split_pair(value):
    high = value.astype(BF)
    return high, (value - high.astype(F32)).astype(BF)


def low_sublanes(shape):
    return lax.broadcasted_iota(jnp.int32, shape, 0) < 4


def pack_columns(adj, kx, ky, even, odd, pair, full, first, last, kxv, kyv, sems):
    cells_x, cells_y, _ = adj.shape
    coefs = [
        pltpu.make_async_copy(kx, kxv, sems.at[2]),
        pltpu.make_async_copy(ky, kyv, sems.at[3]),
    ]
    strips = [
        pltpu.make_async_copy(adj.at[:, pl.ds(0, 8)], first, sems.at[0]),
        pltpu.make_async_copy(adj.at[:, pl.ds(cells_y - 8, 8)], last, sems.at[1]),
    ]
    for copy in coefs + strips:
        copy.start()
    is_last_x = jnp.logical_and(
        lax.axis_index("g") == lax.axis_size("g") - 1, parity_x() == 1
    )
    is_last_y = lax.axis_index("gy") == lax.axis_size("gy") - 1
    end_x = jnp.where(is_last_x, cells_x - 1, -1)
    end_y = jnp.where(is_last_y, cells_y - 1, -1)
    row = lax.broadcasted_iota(jnp.int32, (cells_x, cells_y), 0)
    col = lax.broadcasted_iota(jnp.int32, (cells_x, cells_y), 1)
    for copy in coefs:
        copy.wait()
    conx = jnp.where(row == end_x, 0.0, kxv[...])
    cony = jnp.where(col == end_y, 0.0, kyv[...])
    full[:, :cells_y] = conx
    full[:, cells_y:] = cony
    pieces = jnp.concatenate([*split_pair(conx), *split_pair(cony)], axis=1)
    pair[...] = pieces
    even[64:80, :] = pieces
    odd[64:80, :] = pieces
    for copy in strips:
        copy.wait()
    is_even = parity_y() == 0
    for i in range(8):
        a, b = first[i].astype(F32), first[i + 8].astype(F32)
        c, d = last[i].astype(F32), last[i + 8].astype(F32)
        low = low_sublanes(a.shape)
        leftward = jnp.where(low, a, pltpu.roll(b, 4, 0))
        rightward = jnp.where(low, pltpu.roll(c, 4, 0), d)
        even[8 * i : 8 * i + 8, :] = jnp.where(is_even, rightward, leftward).astype(BF)
        odd[8 * i : 8 * i + 8, :] = jnp.where(is_even, leftward, rightward).astype(BF)


def side_bases(cells_x):
    is_even = parity_x() == 0
    return jnp.where(is_even, cells_x - 4, 0), jnp.where(is_even, 0, cells_x - 4)


def order_weights(order, weights, out, ready, spread):
    picks, cells_x, cells_y = weights.shape
    core = parity_x()
    ready[...] = jnp.zeros_like(ready)

    @pl.loop(0, picks // 32)
    def _(g):
        for c in range(2):
            base = jnp.bitwise_xor(core, c) * (picks // 2) + g * 16
            for s in range(16):
                pick = order[g * 32 + c * 16 + s]
                spread[pl.ds(base + s, cells_x, stride=PITCH), :] = weights[pick].astype(F32)

    @pl.loop(0, cells_x)
    def _(i):
        block = spread[pl.ds(pl.multiple_of(i * PITCH, 8), picks), :]
        out[:, pl.ds(pl.multiple_of(i * cells_y, cells_y), cells_y)] = block.astype(BF)


def pack_rows(adj, pair, y_even, y_odd, ready, even, odd, halo, kh, sems):
    cells_x, cells_y, _ = adj.shape
    del ready
    is_even = parity_x() == 0
    base_even, base_odd = side_bases(cells_x)
    copies = []
    for k in range(4):
        for n, (base, out) in enumerate(((base_even, even), (base_odd, odd))):
            copies.append(
                pltpu.make_async_copy(
                    adj.at[base + k], out.at[pl.ds(k * cells_y, cells_y)], sems.at[2 * k + n]
                )
            )
    for copy in copies:
        copy.start()
    y_is_even = parity_y() == 0
    for i in range(8):
        e, o = y_even[8 * i : 8 * i + 8, :].astype(F32), y_odd[8 * i : 8 * i + 8, :].astype(F32)
        right, left = jnp.where(y_is_even, e, o), jnp.where(y_is_even, o, e)
        low = low_sublanes(e.shape)
        halo[i] = jnp.where(low, right, pltpu.roll(left, 4, 0)).astype(BF)
        halo[i + 8] = jnp.where(low, pltpu.roll(right, 4, 0), left).astype(BF)
    e, o = y_even[64:80, :].astype(F32), y_odd[64:80, :].astype(F32)
    right, left = jnp.where(y_is_even, e, o), jnp.where(y_is_even, o, e)
    lane = lax.broadcasted_iota(jnp.int32, (cells_x, 128), 1)
    parts = []
    for n in range(4):
        span = slice(128 * n, 128 * n + 128)
        parts.append(jnp.where(lane < 4, right[:, span], pltpu.roll(left[:, span], 8, 1)))
    kh[:, :128] = parts[0] + parts[1]
    kh[:, 128:] = parts[2] + parts[3]
    side = jnp.concatenate(parts, axis=1)
    own = pair[...].astype(F32)
    tail = 4 * cells_y + 32
    for base, out, flag in ((base_even, even, is_even), (base_odd, odd, jnp.logical_not(is_even))):
        for k in range(4):
            out[4 * cells_y + 8 * k : 4 * cells_y + 8 * k + 8, :] = halo[base + k]
        out[tail : tail + 8, :] = jnp.where(flag, own[8:], own[:8]).astype(BF)
        out[tail + 8 : tail + 16, :] = jnp.where(flag, side[8:], side[:8]).astype(BF)
    for copy in copies:
        copy.wait()


def put(dst, r, own, side):
    lanes, _, depth, _ = dst.shape
    wrap = depth - 8
    for n in range(lanes):
        span = slice(128 * n, 128 * n + 128)
        dst[n, r, 8 : wrap - 8, :] = own[:, span]
        dst[n, r, wrap - 8 : wrap, :] = side[:, span]
        dst[n, r, 0:8, :] = side[:, span]
        dst[n, r, wrap : wrap + 8, :] = own[:8, span]


def put_coef(dst, r, own, side):
    a = jnp.broadcast_to(own, (own.shape[0], 128))
    b = jnp.broadcast_to(side, (8, 128))
    wrap = dst.shape[1] - 8
    dst[r, 8 : wrap - 8, :] = a
    dst[r, wrap - 8 : wrap, :] = b
    dst[r, 0:8, :] = b


def coefs_at(get_rest, get_up, get_down, get_y, q):
    s = pl.ds(8 + 8 * q, 8)
    (a, i), (b, j), (c, k), (d, m) = get_rest, get_up, get_down, get_y
    return a[i, s, :], b[j, s, :], c[k, s, :], d[m, s, :], d[m, pl.ds(7 + 8 * q, 8), :]


def cell(above, mid, below, q, n, coefs):
    rest, up, down, right, left = coefs
    p = 8 + 8 * q
    (a, i), (b, j), (c, k) = above, mid, below
    total = rest * b[n, j, pl.ds(p, 8), :] + up * a[n, i, pl.ds(p, 8), :]
    total = total + down * c[n, k, pl.ds(p, 8), :]
    total = total + right * b[n, j, pl.ds(p + 1, 8), :]
    return total + left * b[n, j, pl.ds(p - 1, 8), :]


def store(dst, r, q, n, tiles, value):
    dst[n, r, pl.ds(8 + 8 * q, 8), :] = value
    if q == 0:
        dst[n, r, pl.ds(8 + 8 * tiles, 8), :] = value
    if q == tiles - 1:
        dst[n, r, pl.ds(0, 8), :] = value


def rest_of(dst, row, edge_up, edge_down, cond_y, tiles):
    for q in range(tiles):
        _, up, down, right, left = coefs_at((dst, row), edge_up, edge_down, cond_y, q)
        dst[row, pl.ds(8 + 8 * q, 8), :] = 1.0 - (up + down + right + left)


def step_row(above, mid, below, coef_refs, dst, r, tiles, lanes):
    for q in range(tiles):
        coefs = coefs_at(*coef_refs, q)
        for n in range(lanes):
            store(dst, r, q, n, tiles, cell(above, mid, below, q, n, coefs))


def last_row(above, mid, below, coef_refs, out, r, tiles, lanes):
    for q in range(0, tiles - 1, 2):
        ca, cb = coefs_at(*coef_refs, q), coefs_at(*coef_refs, q + 1)
        for n in range(lanes):
            pair = [cell(above, mid, below, q, n, ca), cell(above, mid, below, q + 1, n, cb)]
            new = jnp.concatenate(pair, axis=0).astype(BF)
            out[r, pl.ds(8 * q, 16), pl.ds(128 * n, 128)] = new


def inner(adj, halo, full, kh, mid, u0, u1, u2, u3, cc, cx, cy):
    cells_x, cells_y, cols = adj.shape
    tiles, lanes = cells_y // 8 + 1, cols // 128

    @pl.loop(0, cells_x)
    def _(i):
        put(u0, i, adj[i].astype(F32), halo[i].astype(F32))

    for dst, n in ((cx, 0), (cy, 1)):
        own, side = full[:, 128 * n : 128 * n + 128].T, kh[:, 128 * n : 128 * n + 128].T
        for r in range(cells_x):
            put_coef(dst, r, own[:, r : r + 1], side[:8, r : r + 1])

    @pl.loop(1, cells_x - 1)
    def _(r):
        rest_of(cc, r, (cx, r - 1), (cx, r), (cy, r), tiles)

    levels = (u0, u1, u2, u3)
    for step in range(STEPS):
        src = levels[step]

        @pl.loop(1 + step, cells_x - 1 - step)
        def _(r, src=src, step=step):
            rows = (src, r - 1), (src, r), (src, r + 1)
            refs = (cc, r), (cx, r - 1), (cx, r), (cy, r)
            if step == STEPS - 1:
                last_row(*rows, refs, mid, r - 4, tiles, lanes)
            else:
                step_row(*rows, refs, levels[step + 1], r, tiles, lanes)


def side_rows(below, got, levels, coefs, held, lx, ly, lc, out):
    cc, cx, cy = coefs
    lanes, cells_x, depth, _ = levels[0].shape
    tiles = depth // 8 - 2
    cells_y = 8 * (tiles - 1)
    tail = 4 * cells_y + 32
    at = lambda k: cells_x - 1 - k if below else k
    sent = lambda k: -1 - k if below else k + 4
    for k in range(-4, 0):
        i = sent(k)
        own = got[cells_y * i : cells_y * (i + 1), :].astype(F32)
        side = got[4 * cells_y + 8 * i : 4 * cells_y + 8 * i + 8, :].astype(F32)
        put(held[0], k + 4, own, side)
    tile_o = got[tail : tail + 8, :].astype(F32)
    tile_h = got[tail + 8 : tail + 16, :].astype(F32)
    for dst, n in ((lx, 0), (ly, 2)):
        both = [t[:, 128 * n : 128 * n + 128] + t[:, 128 * n + 128 : 128 * n + 256] for t in (tile_o, tile_h)]
        own, side = both[0].T, both[1].T
        for k in range(-4, 0):
            r = sent(k) if below else sent(k) + 4
            put_coef(dst, k + 4, own[:, r : r + 1], side[:8, r : r + 1])

    def row(level, k):
        return (held[level], k + 4 - level) if k < level else (levels[level], at(k))

    def edge(k):
        if below:
            return (cx, at(k)) if k >= 0 else (lx, k + 4)
        return (cx, at(k) - 1) if k >= 1 else (lx, k + 3)

    def cond_y(k):
        return (cy, at(k)) if k >= 0 else (ly, k + 4)

    for k in range(-3, 1):
        rest_of(lc, k + 3, edge(k), edge(k + 1), cond_y(k), tiles)
    for level in range(STEPS):
        for k in range(level - 3, level + 1):
            rows = row(level, k - 1), row(level, k), row(level, k + 1)
            rest = (cc, at(k)) if k >= 1 else (lc, k + 3)
            refs = rest, edge(k), edge(k + 1), cond_y(k)
            if level == STEPS - 1:
                last_row(*rows, refs, out, 3 - k if below else k, tiles, lanes)
            else:
                step_row(*rows, refs, held[level + 1], k + 3 - level, tiles, lanes)


def first_side(got, u0, u1, u2, u3, cc, cx, cy, weights, mid, out, acc, h0, h1, h2, h3, lx, ly, lc):
    args = got, (u0, u1, u2, u3), (cc, cx, cy), (h0, h1, h2, h3), lx, ly, lc, out
    is_even = parity_x() == 0
    pl.when(is_even)(lambda: side_rows(True, *args))
    pl.when(jnp.logical_not(is_even))(lambda: side_rows(False, *args))
    _, cells_y, cols = mid.shape
    wide = 4 * cells_y
    base = pl.multiple_of(jnp.where(is_even, 3 * wide, 0), wide)
    acc[...] = jnp.dot(
        weights[:, wide : 3 * wide], mid[...].reshape(2 * wide, cols), preferred_element_type=F32
    ) + jnp.dot(
        weights[:, pl.ds(base, wide)], out[...].reshape(wide, cols), preferred_element_type=F32
    )


def second_side(
    got, u0, u1, u2, u3, cc, cx, cy, weights, mid, first, acc, out, send, keep,
    second, h0, h1, h2, h3, lx, ly, lc, sems,
):
    is_even = parity_x() == 0
    base_first, base_second = side_bases(u0.shape[1])
    early = [
        pltpu.make_async_copy(mid, out.at[pl.ds(4, mid.shape[0])], sems.at[0]),
        pltpu.make_async_copy(first, out.at[pl.ds(base_first, 4)], sems.at[1]),
    ]
    for copy in early:
        copy.start()
    args = got, (u0, u1, u2, u3), (cc, cx, cy), (h0, h1, h2, h3), lx, ly, lc, second
    pl.when(is_even)(lambda: side_rows(False, *args))
    pl.when(jnp.logical_not(is_even))(lambda: side_rows(True, *args))
    late = pltpu.make_async_copy(second, out.at[pl.ds(base_second, 4)], sems.at[2])
    late.start()
    _, cells_y, cols = mid.shape
    wide = 4 * cells_y
    base = pl.multiple_of(base_second * cells_y, wide)
    half = weights.shape[0] // 2
    field = second[...].reshape(wide, cols)
    for dst, rows in ((send, slice(half, 2 * half)), (keep, slice(0, half))):
        dst[...] = acc[rows, :] + jnp.dot(
            weights[rows, pl.ds(base, wide)], field, preferred_element_type=F32
        )
    for copy in early + [late]:
        copy.wait()


def pairs_even(peers):
    return [(i, i ^ 1) for i in range(peers)]


def pairs_odd(peers):
    ups = [(i, i + 1) for i in range(1, peers - 1, 2)]
    return ups + [(j, i) for i, j in ups]


def call(kernel, shapes, ins, outs, scratch, limit, flops, **more):
    return pl.pallas_call(
        kernel,
        out_shape=tuple(jax.ShapeDtypeStruct(*s) for s in shapes),
        in_specs=ins,
        out_specs=tuple(outs),
        scratch_shapes=scratch,
        compiler_params=pltpu.CompilerParams(vmem_limit_bytes=limit),
        cost_estimate=pl.CostEstimate(flops=flops, bytes_accessed=0, transcendentals=0),
        **more,
    )


def per_device(adjoint, conduct_x, conduct_y, pick_weights, owner_order):
    cells_x, cells_y, cols = adjoint.shape
    picks = pick_weights.shape[0]
    peers_x, peers_y = lax.axis_size(ALONG), lax.axis_size("gy")
    rows = 4 * cells_y + 32 + 16
    strip = ((80, cols), BF)
    payload = ((rows, cols), BF)
    dma = pltpu.SemaphoreType.DMA

    y_even, y_odd, pair, full = call(
        pack_columns,
        [strip, strip, ((cells_x, 4 * cells_y), BF), ((cells_x, 2 * cells_y), F32)],
        [HBM, HBM, HBM],
        [VMEM] * 4,
        [pltpu.VMEM((cells_x, 8, cols), BF)] * 2 + [pltpu.VMEM((cells_x, cells_y), F32)] * 2 + [dma((4,))],
        59 * MIB,
        1 << 20,
    )(adjoint, conduct_x, conduct_y)
    y_odd = lax.ppermute(y_odd, "gy", pairs_odd(peers_y))
    y_even = lax.ppermute(y_even, "gy", pairs_even(peers_y))

    weights, ready = call(
        order_weights,
        [((picks, cells_x * cells_y), BF), ((8, 128), F32)],
        [SMEM, VMEM],
        [VMEM] * 2,
        [pltpu.VMEM((cells_x * PITCH, cells_y), F32)],
        8 * MIB,
        1 << 27,
    )(owner_order, pick_weights)

    x_even, x_odd, halo, kh = call(
        pack_rows,
        [payload, payload, ((cells_x, 8, cols), BF), ((cells_x, 256), F32)],
        [HBM, VMEM, VMEM, VMEM, VMEM],
        [VMEM] * 4,
        [dma((8,))],
        8 * MIB,
        1 << 20,
    )(adjoint, pair, y_even, y_odd, ready)
    x_odd = lax.ppermute(x_odd, ALONG, pairs_odd(peers_x))
    x_even = lax.ppermute(x_even, ALONG, pairs_even(peers_x))

    depth = cells_y + 24
    level = ((cols // 128, cells_x, depth, 128), F32)
    wide = ((cells_x, depth, 128), F32)
    mid, *state = call(
        inner,
        [((8, cells_y, cols), BF)] + [level] * 4 + [wide] * 3,
        [VMEM] * 4,
        [VMEM] * 8,
        [],
        8 * MIB,
        1 << 28,
    )(adjoint, halo, full, kh)
    side = [pltpu.VMEM((cols // 128, 4, depth, 128), F32)] * 4 + [pltpu.VMEM((4, depth, 128), F32)] * 3
    edge = ((4, cells_y, cols), BF)
    first, acc = call(
        first_side,
        [edge, ((picks, cols), F32)],
        [VMEM] * 10,
        [VMEM] * 2,
        side,
        16 * MIB,
        1 << 27,
    )(x_even, *state, weights, mid)
    smoothed, send, keep = call(
        second_side,
        [(adjoint.shape, BF), ((picks // 2, cols), F32), ((picks // 2, cols), F32)],
        [VMEM] * 12,
        [HBM, VMEM, VMEM],
        [pltpu.VMEM(*edge)] + side + [dma((3,))],
        16 * MIB,
        1 << 27,
    )(x_odd, *state, weights, mid, first, acc)
    other = lax.ppermute(send, "core", [(0, 1), (1, 0)])
    merged = (keep + other).astype(BF).reshape(-1, 2, cols)
    arrived = lax.all_to_all(merged, ("g", "gy"), split_axis=0, concat_axis=0, tiled=True)
    return smoothed, arrived.astype(F32).sum(axis=0)


def solution(mesh):
    peers_x, peers_y = mesh.devices.shape
    split = Mesh(mesh.devices.reshape(peers_x // 2, 2, peers_y), ("g", "core", "gy"))
    return jax.shard_map(
        per_device,
        mesh=split,
        in_specs=(P(ALONG, "gy", None), P(ALONG, "gy"), P(ALONG, "gy"), P(None, ALONG, "gy"), P()),
        out_specs=(P(ALONG, "gy", None), P(("g", "core", "gy"), None)),
        check_vma=False,
    )
```

```python
import jax
import jax.numpy as jnp
from jax import lax
from jax.experimental import pallas as pl
from jax.experimental.pallas import tpu as pltpu
from jax.sharding import Mesh
from jax.sharding import PartitionSpec as P

STEPS = 4
BF = jnp.bfloat16
F32 = jnp.float32
VMEM = pl.BlockSpec(memory_space=pltpu.VMEM)
SMEM = pl.BlockSpec(memory_space=pltpu.SMEM)
HBM = pl.BlockSpec(memory_space=pltpu.HBM)
ANY = pl.BlockSpec(memory_space=pl.ANY)
MIB = 1024 * 1024
ALONG = ("g", "core")
PITCH = 520


def parity_x():
    return lax.axis_index("core")


def parity_y():
    return lax.rem(lax.axis_index("gy"), 2)


def split_pair(value):
    high = value.astype(BF)
    return high, (value - high.astype(F32)).astype(BF)


def low_sublanes(shape):
    return lax.broadcasted_iota(jnp.int32, shape, 0) < 4


def pack_columns(first, last, conduct, even, odd, pair, full):
    _, cells_x, cells_y = conduct.shape
    is_last_x = jnp.logical_and(
        lax.axis_index("g") == lax.axis_size("g") - 1, parity_x() == 1
    )
    is_last_y = lax.axis_index("gy") == lax.axis_size("gy") - 1
    end_x = jnp.where(is_last_x, cells_x - 1, -1)
    end_y = jnp.where(is_last_y, cells_y - 1, -1)
    row = lax.broadcasted_iota(jnp.int32, (cells_x, cells_y), 0)
    col = lax.broadcasted_iota(jnp.int32, (cells_x, cells_y), 1)
    conx = jnp.where(row == end_x, 0.0, conduct[0])
    cony = jnp.where(col == end_y, 0.0, conduct[1])
    full[:, :cells_y] = conx
    full[:, cells_y:] = cony
    pieces = jnp.concatenate([*split_pair(conx), *split_pair(cony)], axis=1)
    pair[...] = pieces
    even[64:80, :] = pieces
    odd[64:80, :] = pieces
    is_even = parity_y() == 0
    for i in range(8):
        a, b = first[i].astype(F32), first[i + 8].astype(F32)
        c, d = last[i].astype(F32), last[i + 8].astype(F32)
        low = low_sublanes(a.shape)
        leftward = jnp.where(low, a, pltpu.roll(b, 4, 0))
        rightward = jnp.where(low, pltpu.roll(c, 4, 0), d)
        even[8 * i : 8 * i + 8, :] = jnp.where(is_even, rightward, leftward).astype(BF)
        odd[8 * i : 8 * i + 8, :] = jnp.where(is_even, leftward, rightward).astype(BF)


def side_bases(cells_x):
    is_even = parity_x() == 0
    return jnp.where(is_even, cells_x - 4, 0), jnp.where(is_even, 0, cells_x - 4)


def order_weights(order, weights, adj, out, even, odd, spread):
    picks, cells_x, cells_y = weights.shape
    core = parity_x()
    for k in range(4):
        for base, dst in zip(side_bases(cells_x), (even, odd)):
            dst[k * cells_y : (k + 1) * cells_y, :] = adj[base + k]

    @pl.loop(0, picks // 32)
    def _(g):
        for c in range(2):
            base = jnp.bitwise_xor(core, c) * (picks // 2) + g * 16
            for s in range(16):
                pick = order[g * 32 + c * 16 + s]
                spread[pl.ds(base + s, cells_x, stride=PITCH), :] = weights[pick].astype(F32)

    @pl.loop(0, cells_x)
    def _(i):
        block = spread[pl.ds(pl.multiple_of(i * PITCH, 8), picks), :]
        out[:, pl.ds(pl.multiple_of(i * cells_y, cells_y), cells_y)] = block.astype(BF)


def pack_rows(even_in, odd_in, pair, y_even, y_odd, even, odd, halo, kh, tail_even, tail_odd, sems):
    del even_in, odd_in
    cells_x = halo.shape[0]
    is_even = parity_x() == 0
    base_even, base_odd = side_bases(cells_x)
    y_is_even = parity_y() == 0
    for i in range(8):
        e, o = y_even[8 * i : 8 * i + 8, :].astype(F32), y_odd[8 * i : 8 * i + 8, :].astype(F32)
        right, left = jnp.where(y_is_even, e, o), jnp.where(y_is_even, o, e)
        low = low_sublanes(e.shape)
        halo[i] = jnp.where(low, right, pltpu.roll(left, 4, 0)).astype(BF)
        halo[i + 8] = jnp.where(low, pltpu.roll(right, 4, 0), left).astype(BF)
    e, o = y_even[64:80, :].astype(F32), y_odd[64:80, :].astype(F32)
    right, left = jnp.where(y_is_even, e, o), jnp.where(y_is_even, o, e)
    lane = lax.broadcasted_iota(jnp.int32, (cells_x, 128), 1)
    parts = []
    for n in range(4):
        span = slice(128 * n, 128 * n + 128)
        parts.append(jnp.where(lane < 4, right[:, span], pltpu.roll(left[:, span], 8, 1)))
    kh[:, :128] = parts[0] + parts[1]
    kh[:, 128:] = parts[2] + parts[3]
    side = jnp.concatenate(parts, axis=1)
    own = pair[...].astype(F32)
    is_odd = jnp.logical_not(is_even)
    copies = []
    for n, (base, out, tail, flag) in enumerate(
        ((base_even, even, tail_even, is_even), (base_odd, odd, tail_odd, is_odd))
    ):
        for k in range(4):
            tail[8 * k : 8 * k + 8, :] = halo[base + k]
        tail[32:40, :] = jnp.where(flag, own[8:], own[:8]).astype(BF)
        tail[40:48, :] = jnp.where(flag, side[8:], side[:8]).astype(BF)
        copies.append(pltpu.make_async_copy(tail, out.at[pl.ds(out.shape[0] - 48, 48)], sems.at[n]))
        copies[-1].start()
    for copy in copies:
        copy.wait()


def put(dst, r, own, side):
    lanes, _, depth, _ = dst.shape
    wrap = depth - 8
    for n in range(lanes):
        span = slice(128 * n, 128 * n + 128)
        dst[n, r, 8 : wrap - 8, :] = own[:, span]
        dst[n, r, wrap - 8 : wrap, :] = side[:, span]
        dst[n, r, 0:8, :] = side[:, span]
        dst[n, r, wrap : wrap + 8, :] = own[:8, span]


def put_coef(dst, r, own, side):
    a = jnp.broadcast_to(own, (own.shape[0], 128))
    b = jnp.broadcast_to(side, (8, 128))
    wrap = dst.shape[1] - 8
    dst[r, 8 : wrap - 8, :] = a
    dst[r, wrap - 8 : wrap, :] = b
    dst[r, 0:8, :] = b


def coefs_at(get_rest, get_up, get_down, get_y, q):
    s = pl.ds(8 + 8 * q, 8)
    (a, i), (b, j), (c, k), (d, m) = get_rest, get_up, get_down, get_y
    return a[i, s, :], b[j, s, :], c[k, s, :], d[m, s, :], d[m, pl.ds(7 + 8 * q, 8), :]


def cell(above, mid, below, q, n, coefs):
    rest, up, down, right, left = coefs
    p = 8 + 8 * q
    (a, i), (b, j), (c, k) = above, mid, below
    total = rest * b[n, j, pl.ds(p, 8), :] + up * a[n, i, pl.ds(p, 8), :]
    total = total + down * c[n, k, pl.ds(p, 8), :]
    total = total + right * b[n, j, pl.ds(p + 1, 8), :]
    return total + left * b[n, j, pl.ds(p - 1, 8), :]


def store(dst, r, q, n, tiles, value):
    dst[n, r, pl.ds(8 + 8 * q, 8), :] = value
    if q == 0:
        dst[n, r, pl.ds(8 + 8 * tiles, 8), :] = value
    if q == tiles - 1:
        dst[n, r, pl.ds(0, 8), :] = value


def rest_of(dst, row, edge_up, edge_down, cond_y, tiles):
    for q in range(tiles):
        _, up, down, right, left = coefs_at((dst, row), edge_up, edge_down, cond_y, q)
        dst[row, pl.ds(8 + 8 * q, 8), :] = 1.0 - (up + down + right + left)


def step_row(above, mid, below, coef_refs, dst, r, tiles, lanes):
    for q in range(tiles):
        coefs = coefs_at(*coef_refs, q)
        for n in range(lanes):
            store(dst, r, q, n, tiles, cell(above, mid, below, q, n, coefs))


def last_row(above, mid, below, coef_refs, out, r, tiles, lanes):
    for q in range(0, tiles - 1, 2):
        ca, cb = coefs_at(*coef_refs, q), coefs_at(*coef_refs, q + 1)
        for n in range(lanes):
            pair = [cell(above, mid, below, q, n, ca), cell(above, mid, below, q + 1, n, cb)]
            new = jnp.concatenate(pair, axis=0).astype(BF)
            out[r, pl.ds(8 * q, 16), pl.ds(128 * n, 128)] = new


def inner(adj, halo, full, kh, mid, u0, u1, u2, u3, cc, cx, cy):
    cells_x, cells_y, cols = adj.shape
    tiles, lanes = cells_y // 8 + 1, cols // 128

    turned = [
        (dst, full[:, 128 * n : 128 * n + 128].T, kh[:, 128 * n : 128 * n + 128].T)
        for n, dst in enumerate((cx, cy))
    ]
    for r in range(cells_x):
        put(u0, r, adj[r].astype(F32), halo[r].astype(F32))
        for dst, own, side in turned:
            put_coef(dst, r, own[:, r : r + 1], side[:8, r : r + 1])

    @pl.loop(1, cells_x - 1)
    def _(r):
        rest_of(cc, r, (cx, r - 1), (cx, r), (cy, r), tiles)

    levels = (u0, u1, u2, u3)
    for step in range(STEPS):
        src = levels[step]

        @pl.loop(1 + step, cells_x - 1 - step)
        def _(r, src=src, step=step):
            rows = (src, r - 1), (src, r), (src, r + 1)
            refs = (cc, r), (cx, r - 1), (cx, r), (cy, r)
            if step == STEPS - 1:
                last_row(*rows, refs, mid, r - 4, tiles, lanes)
            else:
                step_row(*rows, refs, levels[step + 1], r, tiles, lanes)


def side_rows(below, got, levels, coefs, held, lx, ly, lc, out):
    cc, cx, cy = coefs
    lanes, cells_x, depth, _ = levels[0].shape
    tiles = depth // 8 - 2
    cells_y = 8 * (tiles - 1)
    tail = 4 * cells_y + 32
    at = lambda k: cells_x - 1 - k if below else k
    sent = lambda k: -1 - k if below else k + 4
    for k in range(-4, 0):
        i = sent(k)
        own = got[cells_y * i : cells_y * (i + 1), :].astype(F32)
        side = got[4 * cells_y + 8 * i : 4 * cells_y + 8 * i + 8, :].astype(F32)
        put(held[0], k + 4, own, side)
    tile_o = got[tail : tail + 8, :].astype(F32)
    tile_h = got[tail + 8 : tail + 16, :].astype(F32)
    for dst, n in ((lx, 0), (ly, 2)):
        both = [t[:, 128 * n : 128 * n + 128] + t[:, 128 * n + 128 : 128 * n + 256] for t in (tile_o, tile_h)]
        own, side = both[0].T, both[1].T
        for k in range(-4, 0):
            r = sent(k) if below else sent(k) + 4
            put_coef(dst, k + 4, own[:, r : r + 1], side[:8, r : r + 1])

    def row(level, k):
        return (held[level], k + 4 - level) if k < level else (levels[level], at(k))

    def edge(k):
        if below:
            return (cx, at(k)) if k >= 0 else (lx, k + 4)
        return (cx, at(k) - 1) if k >= 1 else (lx, k + 3)

    def cond_y(k):
        return (cy, at(k)) if k >= 0 else (ly, k + 4)

    for k in range(-3, 1):
        rest_of(lc, k + 3, edge(k), edge(k + 1), cond_y(k), tiles)
    for level in range(STEPS):
        for k in range(level - 3, level + 1):
            rows = row(level, k - 1), row(level, k), row(level, k + 1)
            rest = (cc, at(k)) if k >= 1 else (lc, k + 3)
            refs = rest, edge(k), edge(k + 1), cond_y(k)
            if level == STEPS - 1:
                last_row(*rows, refs, out, 3 - k if below else k, tiles, lanes)
            else:
                step_row(*rows, refs, held[level + 1], k + 3 - level, tiles, lanes)


def first_side(got, u0, u1, u2, u3, cc, cx, cy, weights, mid, out, acc, h0, h1, h2, h3, lx, ly, lc):
    args = got, (u0, u1, u2, u3), (cc, cx, cy), (h0, h1, h2, h3), lx, ly, lc, out
    is_even = parity_x() == 0
    pl.when(is_even)(lambda: side_rows(True, *args))
    pl.when(jnp.logical_not(is_even))(lambda: side_rows(False, *args))
    _, cells_y, cols = mid.shape
    wide = 4 * cells_y
    base = pl.multiple_of(jnp.where(is_even, 3 * wide, 0), wide)
    acc[...] = jnp.dot(
        weights[:, wide : 3 * wide], mid[...].reshape(2 * wide, cols), preferred_element_type=F32
    ) + jnp.dot(
        weights[:, pl.ds(base, wide)], out[...].reshape(wide, cols), preferred_element_type=F32
    )


def second_side(
    got, u0, u1, u2, u3, cc, cx, cy, weights, acc, out, send, h0, h1, h2, h3, lx, ly, lc
):
    is_even = parity_x() == 0
    args = got, (u0, u1, u2, u3), (cc, cx, cy), (h0, h1, h2, h3), lx, ly, lc, out
    pl.when(is_even)(lambda: side_rows(False, *args))
    pl.when(jnp.logical_not(is_even))(lambda: side_rows(True, *args))
    add_side(slice(weights.shape[0] // 2, weights.shape[0]), out, weights, acc, send)


def add_side(rows, side, weights, acc, dst):
    _, cells_y, cols = side.shape
    wide = 4 * cells_y
    _, base = side_bases(weights.shape[1] // cells_y)
    dst[...] = acc[rows, :] + jnp.dot(
        weights[rows, pl.ds(pl.multiple_of(base * cells_y, wide), wide)],
        side[...].reshape(wide, cols),
        preferred_element_type=F32,
    )


def finish(first, mid, second, weights, acc, out, keep, sems):
    base_first, base_second = side_bases(out.shape[0])
    copies = [
        pltpu.make_async_copy(mid, out.at[pl.ds(4, mid.shape[0])], sems.at[0]),
        pltpu.make_async_copy(first, out.at[pl.ds(base_first, 4)], sems.at[1]),
        pltpu.make_async_copy(second, out.at[pl.ds(base_second, 4)], sems.at[2]),
    ]
    for copy in copies:
        copy.start()
    add_side(slice(0, weights.shape[0] // 2), second, weights, acc, keep)
    for copy in copies:
        copy.wait()


def pairs_even(peers):
    return [(i, i ^ 1) for i in range(peers)]


def pairs_odd(peers):
    ups = [(i, i + 1) for i in range(1, peers - 1, 2)]
    return ups + [(j, i) for i, j in ups]


def call(kernel, shapes, ins, outs, scratch, limit, flops, **more):
    return pl.pallas_call(
        kernel,
        out_shape=tuple(jax.ShapeDtypeStruct(*s) for s in shapes),
        in_specs=ins,
        out_specs=tuple(outs),
        scratch_shapes=scratch,
        compiler_params=pltpu.CompilerParams(vmem_limit_bytes=limit),
        cost_estimate=pl.CostEstimate(flops=flops, bytes_accessed=0, transcendentals=0),
        **more,
    )


def per_device(adjoint, conduct_x, conduct_y, pick_weights, owner_order):
    cells_x, cells_y, cols = adjoint.shape
    picks = pick_weights.shape[0]
    peers_x, peers_y = lax.axis_size(ALONG), lax.axis_size("gy")
    rows = 4 * cells_y + 32 + 16
    strip = ((80, cols), BF)
    payload = ((rows, cols), BF)
    dma = pltpu.SemaphoreType.DMA

    y_even, y_odd, pair, full = call(
        pack_columns,
        [strip, strip, ((cells_x, 4 * cells_y), BF), ((cells_x, 2 * cells_y), F32)],
        [VMEM] * 3,
        [VMEM] * 4,
        [],
        4 * MIB,
        1 << 33,
    )(adjoint[:, :8], adjoint[:, cells_y - 8 :], jnp.stack([conduct_x, conduct_y]))
    y_odd = lax.ppermute(y_odd, "gy", pairs_odd(peers_y))
    y_even = lax.ppermute(y_even, "gy", pairs_even(peers_y))

    weights, x_even, x_odd = call(
        order_weights,
        [((picks, cells_x * cells_y), BF), payload, payload],
        [SMEM, VMEM, VMEM],
        [VMEM] * 3,
        [pltpu.VMEM((cells_x * PITCH, cells_y), F32)],
        8 * MIB,
        1 << 27,
    )(owner_order, pick_weights, adjoint)

    x_even, x_odd, halo, kh = call(
        pack_rows,
        [payload, payload, ((cells_x, 8, cols), BF), ((cells_x, 256), F32)],
        [ANY, ANY, VMEM, VMEM, VMEM],
        [ANY, ANY, VMEM, VMEM],
        [pltpu.VMEM((48, cols), BF)] * 2 + [dma((2,))],
        4 * MIB,
        1 << 20,
        input_output_aliases={0: 0, 1: 1},
    )(x_even, x_odd, pair, y_even, y_odd)
    x_odd = lax.ppermute(x_odd, ALONG, pairs_odd(peers_x))
    x_even = lax.ppermute(x_even, ALONG, pairs_even(peers_x))

    depth = cells_y + 24
    level = ((cols // 128, cells_x, depth, 128), F32)
    wide = ((cells_x, depth, 128), F32)
    mid, *state = call(
        inner,
        [((8, cells_y, cols), BF)] + [level] * 4 + [wide] * 3,
        [VMEM] * 4,
        [VMEM] * 8,
        [],
        8 * MIB,
        1 << 28,
    )(adjoint, halo, full, kh)
    side = [pltpu.VMEM((cols // 128, 4, depth, 128), F32)] * 4 + [pltpu.VMEM((4, depth, 128), F32)] * 3
    edge = ((4, cells_y, cols), BF)
    first, acc = call(
        first_side,
        [edge, ((picks, cols), F32)],
        [VMEM] * 10,
        [VMEM] * 2,
        side,
        16 * MIB,
        1 << 27,
    )(x_even, *state, weights, mid)
    second, send = call(
        second_side,
        [edge, ((picks // 2, cols), F32)],
        [VMEM] * 10,
        [VMEM] * 2,
        side,
        16 * MIB,
        1 << 27,
    )(x_odd, *state, weights, acc)
    other = lax.ppermute(send, "core", [(0, 1), (1, 0)])
    smoothed, keep = call(
        finish,
        [(adjoint.shape, BF), ((picks // 2, cols), F32)],
        [VMEM] * 5,
        [HBM, VMEM],
        [dma((3,))],
        8 * MIB,
        1 << 27,
    )(first, mid, second, weights, acc)
    merged = (keep + other).astype(BF).reshape(-1, 2, cols)
    arrived = lax.all_to_all(merged, ("g", "gy"), split_axis=0, concat_axis=0, tiled=True)
    return smoothed, arrived.astype(F32).sum(axis=0)


def solution(mesh):
    peers_x, peers_y = mesh.devices.shape
    split = Mesh(mesh.devices.reshape(peers_x // 2, 2, peers_y), ("g", "core", "gy"))
    return jax.shard_map(
        per_device,
        mesh=split,
        in_specs=(P(ALONG, "gy", None), P(ALONG, "gy"), P(ALONG, "gy"), P(None, ALONG, "gy"), P()),
        out_specs=(P(ALONG, "gy", None), P(("g", "core", "gy"), None)),
        check_vma=False,
    )
```

```python
import jax
import jax.numpy as jnp
from jax import lax
from jax.experimental import pallas as pl
from jax.experimental.pallas import tpu as pltpu
from jax.sharding import Mesh
from jax.sharding import PartitionSpec as P

STEPS = 4
BF = jnp.bfloat16
F32 = jnp.float32
VMEM = pl.BlockSpec(memory_space=pltpu.VMEM)
SMEM = pl.BlockSpec(memory_space=pltpu.SMEM)
HBM = pl.BlockSpec(memory_space=pltpu.HBM)
ANY = pl.BlockSpec(memory_space=pl.ANY)
MIB = 1024 * 1024
ALONG = ("g", "core")
PITCH = 520


def parity_x():
    return lax.axis_index("core")


def parity_y():
    return lax.rem(lax.axis_index("gy"), 2)


def split_pair(value):
    high = value.astype(BF)
    return high, (value - high.astype(F32)).astype(BF)


def low_sublanes(shape):
    return lax.broadcasted_iota(jnp.int32, shape, 0) < 4


def pack_columns(first, last, conduct, even, odd, pair, full):
    _, cells_x, cells_y = conduct.shape
    is_last_x = jnp.logical_and(
        lax.axis_index("g") == lax.axis_size("g") - 1, parity_x() == 1
    )
    is_last_y = lax.axis_index("gy") == lax.axis_size("gy") - 1
    end_x = jnp.where(is_last_x, cells_x - 1, -1)
    end_y = jnp.where(is_last_y, cells_y - 1, -1)
    row = lax.broadcasted_iota(jnp.int32, (cells_x, cells_y), 0)
    col = lax.broadcasted_iota(jnp.int32, (cells_x, cells_y), 1)
    conx = jnp.where(row == end_x, 0.0, conduct[0])
    cony = jnp.where(col == end_y, 0.0, conduct[1])
    full[:, :cells_y] = conx
    full[:, cells_y:] = cony
    pieces = jnp.concatenate([*split_pair(conx), *split_pair(cony)], axis=1)
    pair[...] = pieces
    even[64:80, :] = pieces
    odd[64:80, :] = pieces
    is_even = parity_y() == 0
    for i in range(8):
        a, b = first[i].astype(F32), first[i + 8].astype(F32)
        c, d = last[i].astype(F32), last[i + 8].astype(F32)
        low = low_sublanes(a.shape)
        leftward = jnp.where(low, a, pltpu.roll(b, 4, 0))
        rightward = jnp.where(low, pltpu.roll(c, 4, 0), d)
        even[8 * i : 8 * i + 8, :] = jnp.where(is_even, rightward, leftward).astype(BF)
        odd[8 * i : 8 * i + 8, :] = jnp.where(is_even, leftward, rightward).astype(BF)


def side_bases(cells_x):
    is_even = parity_x() == 0
    return jnp.where(is_even, cells_x - 4, 0), jnp.where(is_even, 0, cells_x - 4)


def order_weights(order, weights, adj, out, even, odd, spread):
    picks, cells_x, cells_y = weights.shape
    core = parity_x()
    for k in range(4):
        for base, dst in zip(side_bases(cells_x), (even, odd)):
            dst[k * cells_y : (k + 1) * cells_y, :] = adj[base + k]

    @pl.loop(0, picks // 32)
    def _(g):
        for c in range(2):
            base = jnp.bitwise_xor(core, c) * (picks // 2) + g * 16
            for s in range(16):
                pick = order[g * 32 + c * 16 + s]
                spread[pl.ds(base + s, cells_x, stride=PITCH), :] = weights[pick].astype(F32)

    @pl.loop(0, cells_x)
    def _(i):
        block = spread[pl.ds(pl.multiple_of(i * PITCH, 8), picks), :]
        out[:, pl.ds(pl.multiple_of(i * cells_y, cells_y), cells_y)] = block.astype(BF)


def pack_rows(even_in, odd_in, pair, y_even, y_odd, even, odd, halo, kh, tail_even, tail_odd, sems):
    del even_in, odd_in
    cells_x = halo.shape[0]
    is_even = parity_x() == 0
    base_even, base_odd = side_bases(cells_x)
    y_is_even = parity_y() == 0
    for i in range(8):
        e, o = y_even[8 * i : 8 * i + 8, :].astype(F32), y_odd[8 * i : 8 * i + 8, :].astype(F32)
        right, left = jnp.where(y_is_even, e, o), jnp.where(y_is_even, o, e)
        low = low_sublanes(e.shape)
        halo[i] = jnp.where(low, right, pltpu.roll(left, 4, 0)).astype(BF)
        halo[i + 8] = jnp.where(low, pltpu.roll(right, 4, 0), left).astype(BF)
    e, o = y_even[64:80, :].astype(F32), y_odd[64:80, :].astype(F32)
    right, left = jnp.where(y_is_even, e, o), jnp.where(y_is_even, o, e)
    lane = lax.broadcasted_iota(jnp.int32, (cells_x, 128), 1)
    parts = []
    for n in range(4):
        span = slice(128 * n, 128 * n + 128)
        parts.append(jnp.where(lane < 4, right[:, span], pltpu.roll(left[:, span], 8, 1)))
    kh[:, :128] = parts[0] + parts[1]
    kh[:, 128:] = parts[2] + parts[3]
    side = jnp.concatenate(parts, axis=1)
    own = pair[...].astype(F32)
    is_odd = jnp.logical_not(is_even)
    copies = []
    for n, (base, out, tail, flag) in enumerate(
        ((base_even, even, tail_even, is_even), (base_odd, odd, tail_odd, is_odd))
    ):
        for k in range(4):
            tail[8 * k : 8 * k + 8, :] = halo[base + k]
        tail[32:40, :] = jnp.where(flag, own[8:], own[:8]).astype(BF)
        tail[40:48, :] = jnp.where(flag, side[8:], side[:8]).astype(BF)
        copies.append(pltpu.make_async_copy(tail, out.at[pl.ds(out.shape[0] - 48, 48)], sems.at[n]))
        copies[-1].start()
    for copy in copies:
        copy.wait()


def put(dst, r, own, side):
    lanes, _, depth, _ = dst.shape
    wrap = depth - 8
    for n in range(lanes):
        span = slice(128 * n, 128 * n + 128)
        dst[n, r, 8 : wrap - 8, :] = own[:, span]
        dst[n, r, wrap - 8 : wrap, :] = side[:, span]
        dst[n, r, 0:8, :] = side[:, span]
        dst[n, r, wrap : wrap + 8, :] = own[:8, span]


def put_coef(dst, r, own, side):
    a = jnp.broadcast_to(own, (own.shape[0], 128))
    b = jnp.broadcast_to(side, (8, 128))
    wrap = dst.shape[1] - 8
    dst[r, 8 : wrap - 8, :] = a
    dst[r, wrap - 8 : wrap, :] = b
    dst[r, 0:8, :] = b


def coefs_at(get_rest, get_up, get_down, get_y, q):
    s = pl.ds(8 + 8 * q, 8)
    (a, i), (b, j), (c, k), (d, m) = get_rest, get_up, get_down, get_y
    return a[i, s, :], b[j, s, :], c[k, s, :], d[m, s, :], d[m, pl.ds(7 + 8 * q, 8), :]


def cell(above, mid, below, q, n, coefs):
    rest, up, down, right, left = coefs
    p = 8 + 8 * q
    (a, i), (b, j), (c, k) = above, mid, below
    total = rest * b[n, j, pl.ds(p, 8), :] + up * a[n, i, pl.ds(p, 8), :]
    total = total + down * c[n, k, pl.ds(p, 8), :]
    total = total + right * b[n, j, pl.ds(p + 1, 8), :]
    return total + left * b[n, j, pl.ds(p - 1, 8), :]


def store(dst, r, q, n, tiles, value):
    dst[n, r, pl.ds(8 + 8 * q, 8), :] = value
    if q == 0:
        dst[n, r, pl.ds(8 + 8 * tiles, 8), :] = value
    if q == tiles - 1:
        dst[n, r, pl.ds(0, 8), :] = value


def rest_of(dst, row, edge_up, edge_down, cond_y, tiles):
    for q in range(tiles):
        _, up, down, right, left = coefs_at((dst, row), edge_up, edge_down, cond_y, q)
        dst[row, pl.ds(8 + 8 * q, 8), :] = 1.0 - (up + down + right + left)


def step_row(above, mid, below, coef_refs, dst, r, tiles, lanes):
    for q in range(tiles):
        coefs = coefs_at(*coef_refs, q)
        for n in range(lanes):
            store(dst, r, q, n, tiles, cell(above, mid, below, q, n, coefs))


def last_row(above, mid, below, coef_refs, out, r, tiles, lanes):
    for q in range(0, tiles - 1, 2):
        ca, cb = coefs_at(*coef_refs, q), coefs_at(*coef_refs, q + 1)
        for n in range(lanes):
            pair = [cell(above, mid, below, q, n, ca), cell(above, mid, below, q + 1, n, cb)]
            new = jnp.concatenate(pair, axis=0).astype(BF)
            out[r, pl.ds(8 * q, 16), pl.ds(128 * n, 128)] = new


def inner(adj, halo, full, kh, mid, u0, u1, u2, u3, cc, cx, cy):
    cells_x, cells_y, cols = adj.shape
    tiles, lanes = cells_y // 8 + 1, cols // 128

    turned = [
        (dst, full[:, 128 * n : 128 * n + 128].T, kh[:, 128 * n : 128 * n + 128].T)
        for n, dst in enumerate((cx, cy))
    ]
    for r in range(cells_x):
        put(u0, r, adj[r].astype(F32), halo[r].astype(F32))
        for dst, own, side in turned:
            put_coef(dst, r, own[:, r : r + 1], side[:8, r : r + 1])

    @pl.loop(1, cells_x - 1)
    def _(r):
        rest_of(cc, r, (cx, r - 1), (cx, r), (cy, r), tiles)

    levels = (u0, u1, u2, u3)
    for step in range(STEPS):
        src = levels[step]

        @pl.loop(1 + step, cells_x - 1 - step)
        def _(r, src=src, step=step):
            rows = (src, r - 1), (src, r), (src, r + 1)
            refs = (cc, r), (cx, r - 1), (cx, r), (cy, r)
            if step == STEPS - 1:
                last_row(*rows, refs, mid, r - 4, tiles, lanes)
            else:
                step_row(*rows, refs, levels[step + 1], r, tiles, lanes)


def side_rows(below, got, levels, coefs, held, lx, ly, lc, out):
    cc, cx, cy = coefs
    lanes, cells_x, depth, _ = levels[0].shape
    tiles = depth // 8 - 2
    cells_y = 8 * (tiles - 1)
    tail = 4 * cells_y + 32
    at = lambda k: cells_x - 1 - k if below else k
    sent = lambda k: -1 - k if below else k + 4
    for k in range(-4, 0):
        i = sent(k)
        own = got[cells_y * i : cells_y * (i + 1), :].astype(F32)
        side = got[4 * cells_y + 8 * i : 4 * cells_y + 8 * i + 8, :].astype(F32)
        put(held[0], k + 4, own, side)
    tile_o = got[tail : tail + 8, :].astype(F32)
    tile_h = got[tail + 8 : tail + 16, :].astype(F32)
    for dst, n in ((lx, 0), (ly, 2)):
        both = [t[:, 128 * n : 128 * n + 128] + t[:, 128 * n + 128 : 128 * n + 256] for t in (tile_o, tile_h)]
        own, side = both[0].T, both[1].T
        for k in range(-4, 0):
            r = sent(k) if below else sent(k) + 4
            put_coef(dst, k + 4, own[:, r : r + 1], side[:8, r : r + 1])

    def row(level, k):
        return (held[level], k + 4 - level) if k < level else (levels[level], at(k))

    def edge(k):
        if below:
            return (cx, at(k)) if k >= 0 else (lx, k + 4)
        return (cx, at(k) - 1) if k >= 1 else (lx, k + 3)

    def cond_y(k):
        return (cy, at(k)) if k >= 0 else (ly, k + 4)

    for k in range(-3, 1):
        rest_of(lc, k + 3, edge(k), edge(k + 1), cond_y(k), tiles)
    for level in range(STEPS):
        for k in range(level - 3, level + 1):
            rows = row(level, k - 1), row(level, k), row(level, k + 1)
            rest = (cc, at(k)) if k >= 1 else (lc, k + 3)
            refs = rest, edge(k), edge(k + 1), cond_y(k)
            if level == STEPS - 1:
                last_row(*rows, refs, out, 3 - k if below else k, tiles, lanes)
            else:
                step_row(*rows, refs, held[level + 1], k + 3 - level, tiles, lanes)


def first_side(got, u0, u1, u2, u3, cc, cx, cy, weights, mid, out, acc, h0, h1, h2, h3, lx, ly, lc):
    args = got, (u0, u1, u2, u3), (cc, cx, cy), (h0, h1, h2, h3), lx, ly, lc, out
    is_even = parity_x() == 0
    pl.when(is_even)(lambda: side_rows(True, *args))
    pl.when(jnp.logical_not(is_even))(lambda: side_rows(False, *args))
    _, cells_y, cols = mid.shape
    wide = 4 * cells_y
    base = pl.multiple_of(jnp.where(is_even, 3 * wide, 0), wide)
    acc[...] = jnp.dot(
        weights[:, wide : 3 * wide], mid[...].reshape(2 * wide, cols), preferred_element_type=F32
    ) + jnp.dot(
        weights[:, pl.ds(base, wide)], out[...].reshape(wide, cols), preferred_element_type=F32
    )


def second_side(
    got, u0, u1, u2, u3, cc, cx, cy, weights, acc, out, send, h0, h1, h2, h3, lx, ly, lc
):
    is_even = parity_x() == 0
    args = got, (u0, u1, u2, u3), (cc, cx, cy), (h0, h1, h2, h3), lx, ly, lc, out
    pl.when(is_even)(lambda: side_rows(False, *args))
    pl.when(jnp.logical_not(is_even))(lambda: side_rows(True, *args))
    add_side(slice(weights.shape[0] // 2, weights.shape[0]), out, weights, acc, send)


def add_side(rows, side, weights, acc, dst):
    _, cells_y, cols = side.shape
    wide = 4 * cells_y
    _, base = side_bases(weights.shape[1] // cells_y)
    dst[...] = acc[rows, :] + jnp.dot(
        weights[rows, pl.ds(pl.multiple_of(base * cells_y, wide), wide)],
        side[...].reshape(wide, cols),
        preferred_element_type=F32,
    )


def finish(first, mid, second, weights, acc, out, keep, sems):
    base_first, base_second = side_bases(out.shape[0])
    copies = [
        pltpu.make_async_copy(mid, out.at[pl.ds(4, mid.shape[0])], sems.at[0]),
        pltpu.make_async_copy(first, out.at[pl.ds(base_first, 4)], sems.at[1]),
        pltpu.make_async_copy(second, out.at[pl.ds(base_second, 4)], sems.at[2]),
    ]
    for copy in copies:
        copy.start()
    add_side(slice(0, weights.shape[0] // 2), second, weights, acc, keep)
    for copy in copies:
        copy.wait()


def add_up(parts, out):
    totals = [parts[n].astype(F32) for n in range(8)]
    for m in range(8, parts.shape[0], 8):
        totals = [t + parts[m + n].astype(F32) for n, t in enumerate(totals)]
    while len(totals) > 1:
        totals = [a + b for a, b in zip(totals[::2], totals[1::2])]
    out[...] = totals[0]


def pairs_even(peers):
    return [(i, i ^ 1) for i in range(peers)]


def pairs_odd(peers):
    ups = [(i, i + 1) for i in range(1, peers - 1, 2)]
    return ups + [(j, i) for i, j in ups]


def call(kernel, shapes, ins, outs, scratch, limit, flops, **more):
    return pl.pallas_call(
        kernel,
        out_shape=tuple(jax.ShapeDtypeStruct(*s) for s in shapes),
        in_specs=ins,
        out_specs=tuple(outs),
        scratch_shapes=scratch,
        compiler_params=pltpu.CompilerParams(vmem_limit_bytes=limit),
        cost_estimate=pl.CostEstimate(flops=flops, bytes_accessed=0, transcendentals=0),
        **more,
    )


def per_device(adjoint, conduct_x, conduct_y, pick_weights, owner_order):
    cells_x, cells_y, cols = adjoint.shape
    picks = pick_weights.shape[0]
    peers_x, peers_y = lax.axis_size(ALONG), lax.axis_size("gy")
    rows = 4 * cells_y + 32 + 16
    strip = ((80, cols), BF)
    payload = ((rows, cols), BF)
    dma = pltpu.SemaphoreType.DMA

    y_even, y_odd, pair, full = call(
        pack_columns,
        [strip, strip, ((cells_x, 4 * cells_y), BF), ((cells_x, 2 * cells_y), F32)],
        [VMEM] * 3,
        [VMEM] * 4,
        [],
        4 * MIB,
        1 << 33,
    )(adjoint[:, :8], adjoint[:, cells_y - 8 :], jnp.stack([conduct_x, conduct_y]))
    y_odd = lax.ppermute(y_odd, "gy", pairs_odd(peers_y))
    y_even = lax.ppermute(y_even, "gy", pairs_even(peers_y))

    weights, x_even, x_odd = call(
        order_weights,
        [((picks, cells_x * cells_y), BF), payload, payload],
        [SMEM, VMEM, VMEM],
        [VMEM] * 3,
        [pltpu.VMEM((cells_x * PITCH, cells_y), F32)],
        8 * MIB,
        1 << 27,
    )(owner_order, pick_weights, adjoint)

    x_even, x_odd, halo, kh = call(
        pack_rows,
        [payload, payload, ((cells_x, 8, cols), BF), ((cells_x, 256), F32)],
        [ANY, ANY, VMEM, VMEM, VMEM],
        [ANY, ANY, VMEM, VMEM],
        [pltpu.VMEM((48, cols), BF)] * 2 + [dma((2,))],
        4 * MIB,
        1 << 20,
        input_output_aliases={0: 0, 1: 1},
    )(x_even, x_odd, pair, y_even, y_odd)
    x_odd = lax.ppermute(x_odd, ALONG, pairs_odd(peers_x))
    x_even = lax.ppermute(x_even, ALONG, pairs_even(peers_x))

    depth = cells_y + 24
    level = ((cols // 128, cells_x, depth, 128), F32)
    wide = ((cells_x, depth, 128), F32)
    mid, *state = call(
        inner,
        [((8, cells_y, cols), BF)] + [level] * 4 + [wide] * 3,
        [VMEM] * 4,
        [VMEM] * 8,
        [],
        8 * MIB,
        1 << 28,
    )(adjoint, halo, full, kh)
    side = [pltpu.VMEM((cols // 128, 4, depth, 128), F32)] * 4 + [pltpu.VMEM((4, depth, 128), F32)] * 3
    edge = ((4, cells_y, cols), BF)
    first, acc = call(
        first_side,
        [edge, ((picks, cols), F32)],
        [VMEM] * 10,
        [VMEM] * 2,
        side,
        16 * MIB,
        1 << 27,
    )(x_even, *state, weights, mid)
    second, send = call(
        second_side,
        [edge, ((picks // 2, cols), F32)],
        [VMEM] * 10,
        [VMEM] * 2,
        side,
        16 * MIB,
        1 << 27,
    )(x_odd, *state, weights, acc)
    other = lax.ppermute(send, "core", [(0, 1), (1, 0)])
    smoothed, keep = call(
        finish,
        [(adjoint.shape, BF), ((picks // 2, cols), F32)],
        [VMEM] * 5,
        [HBM, VMEM],
        [dma((3,))],
        8 * MIB,
        1 << 27,
    )(first, mid, second, weights, acc)
    merged = (keep + other).astype(BF).reshape(-1, 2, cols)
    arrived = lax.all_to_all(merged, ("g", "gy"), split_axis=0, concat_axis=0, tiled=True)
    (owned,) = call(
        add_up, [((2, cols), F32)], [VMEM], [VMEM], [], 4 * MIB, 1 << 20
    )(arrived)
    return smoothed, owned


def solution(mesh):
    peers_x, peers_y = mesh.devices.shape
    split = Mesh(mesh.devices.reshape(peers_x // 2, 2, peers_y), ("g", "core", "gy"))
    return jax.shard_map(
        per_device,
        mesh=split,
        in_specs=(P(ALONG, "gy", None), P(ALONG, "gy"), P(ALONG, "gy"), P(None, ALONG, "gy"), P()),
        out_specs=(P(ALONG, "gy", None), P(("g", "core", "gy"), None)),
        check_vma=False,
    )
```
